32 devices in a mesh: dp: 16 (over z, x, core), tensor: 2 (over y).
Axes of the slice: x: 2, y: 2, z: 4, core: 2. Of those that a mesh axis runs over, the one named last changes fastest.
Arguments:
- grad_hidden: bfloat16 [2048, 14336], P('dp', 'tensor'), may hold values from -18 to 18
- gate: bfloat16 [2048, 14336], P('dp', 'tensor'), may hold values from -6 to 6
Outputs:
- factor: float32 [14336, 14336], P('tensor', 'dp')
The draws below stay inside these ranges and needn't reach their ends.
All inputs are finite; a program needn't handle non-finite values.
Results may differ from the reference program's by a relative error of at most 0.0065.
Values may be sent and summed in bfloat16 or wider, within the bound.
No kernel may reach another device: no remote copies, remote signals or barrier semaphores. Data moves between devices by JAX's collectives and lax.ppermute only.
A program may use at most 128 MiB of HBM per device.

```python
import jax
import jax.numpy as jnp
from jax import lax

FF = 14336
TOKENS = 2048


def level_of(rng, extent, split, least, high):
    gain, own = 1.0, jax.random.fold_in(rng, 6)
    for dim, blocks in split:
        draws = jnp.exp(jax.random.uniform(jax.random.fold_in(own, dim), (blocks,), jnp.float32, least / len(split), high / len(split)))
        gain = gain * jnp.repeat(draws, extent[dim] // blocks).reshape([-1 if axis == dim else 1 for axis in range(len(extent))])
    return gain


def bell_draw(stream_key, dims, scale, most, shards=(), dtype=jnp.bfloat16):
    array = jax.random.normal(stream_key, dims, jnp.float32) * scale
    if len(shards) > 0:
        array = level_of(stream_key, dims, shards, -0.22, 0.18) * array
    return jnp.clip(array, min=-most, max=most).astype(dtype)


def setup_inputs(seed: int = 0) -> dict:
    splits = jax.random.split(jax.random.key(seed), 3)
    return {
        "grad_hidden": bell_draw(splits[0], (TOKENS, FF), 3.0, 18.0, ((0, 16), (1, 2))),
        "gate": bell_draw(splits[1], (TOKENS, FF), 1.0, 6.0, ((0, 16), (1, 2))),
    }


def reference(grad_hidden, gate):
    up_grad = (grad_hidden.astype(jnp.float32) * jax.nn.silu(gate.astype(jnp.float32))).astype(jnp.bfloat16)
    wide = up_grad.astype(jnp.float32)
    blocks = wide.reshape(wide.shape[0], FF // 1792 if FF % 1792 == 0 else 1, -1)
    blocks = jnp.transpose(blocks, (1, 0, 2))

    def column_block(piece):
        return jnp.dot(wide.T, piece, precision=lax.Precision.HIGHEST, preferred_element_type=jnp.float32)

    panels = lax.map(column_block, blocks)
    factor = jnp.transpose(panels, (1, 0, 2)).reshape(FF, FF)
    return factor / TOKENS
```

```python
import functools

import jax
import jax.numpy as jnp
from jax import lax
from jax.experimental import pallas as pl
from jax.experimental.pallas import tpu as pltpu
from jax.sharding import PartitionSpec as P

LANES = 128
ANY = pl.BlockSpec(memory_space=pl.ANY)


def gathered(grad_hidden, gate, col_width):
    up_grad = (grad_hidden.astype(jnp.float32) * jax.nn.silu(gate.astype(jnp.float32))).astype(
        jnp.bfloat16
    )
    tensor_count = lax.axis_size("tensor")
    data_count = lax.axis_size("dp")
    ratio = data_count // tensor_count
    data_index = lax.axis_index("dp")
    owner = data_index // ratio
    offset = data_index % ratio * col_width
    contract = (((0,), (0,)), ((), ()))
    total_tokens = up_grad.shape[0] * data_count
    rows_all = lax.all_gather(up_grad, "dp", axis=0, tiled=True)
    panel = lax.dynamic_slice_in_dim(rows_all, offset, col_width, 1)
    slices = lax.all_gather(panel, "tensor", axis=1, tiled=True)
    cols_all = lax.dynamic_slice_in_dim(slices, owner * col_width, col_width, 1)
    summed = lax.dot_general(rows_all, cols_all, contract, preferred_element_type=jnp.float32)
    return summed / total_tokens


def gate_chunk(grad_hidden, gate, dep, col_width, start, width):
    tokens, hidden = grad_hidden.shape
    panels = hidden // col_width

    def body(g_ref, v_ref, dep_ref, o_ref, g_buf, v_buf, sems):
        def copies(m):
            at = pl.ds(m * col_width + start, width)
            return (
                pltpu.make_async_copy(g_ref.at[:, at], g_buf.at[m], sems.at[0, m]),
                pltpu.make_async_copy(v_ref.at[:, at], v_buf.at[m], sems.at[1, m]),
            )

        for m in range(panels):
            for copy in copies(m):
                copy.start()
        for m in range(panels):
            for copy in copies(m):
                copy.wait()
            v = v_buf[m].astype(jnp.float32)
            up = g_buf[m].astype(jnp.float32) * (v * jax.nn.sigmoid(v))
            o_ref[m * width : (m + 1) * width, :] = up.T.astype(jnp.bfloat16)

    return pl.pallas_call(
        body,
        out_shape=jax.ShapeDtypeStruct((panels * width, tokens), jnp.bfloat16),
        in_specs=[ANY, ANY, ANY],
        scratch_shapes=[
            pltpu.VMEM((panels, tokens, width), jnp.bfloat16),
            pltpu.VMEM((panels, tokens, width), jnp.bfloat16),
            pltpu.SemaphoreType.DMA((2, panels)),
        ],
        cost_estimate=pl.CostEstimate(flops=3_000_000_000, transcendentals=0, bytes_accessed=0),
        name=f"gate_{start}",
    )(grad_hidden, gate, dep)


def pick_panel(chunks, panel, width):
    tokens = chunks[0].shape[1]
    count = len(chunks)

    def body(panel_ref, *refs):
        o_ref, sems = refs[count], refs[count + 1]
        at = pl.ds(pl.multiple_of(panel_ref[0] * width, width), width)
        copies = [
            pltpu.make_async_copy(
                refs[i].at[at, :], o_ref.at[:, pl.ds(i * tokens, tokens)], sems.at[i]
            )
            for i in range(count)
        ]
        for copy in copies:
            copy.start()
        for copy in copies:
            copy.wait()

    return pl.pallas_call(
        body,
        out_shape=jax.ShapeDtypeStruct((width, count * tokens), jnp.bfloat16),
        grid_spec=pltpu.PrefetchScalarGridSpec(
            num_scalar_prefetch=1,
            grid=(1,),
            in_specs=[ANY] * count,
            out_specs=pl.BlockSpec((width, count * tokens), lambda i, p: (0, 0)),
            scratch_shapes=[pltpu.SemaphoreType.DMA((count,))],
        ),
        name="pick",
    )(panel, *chunks)


def product(out, rows, cols, panels, widths, col_start, col_width, row_block, scale, name):
    tokens = rows[0][0].shape[1]
    count = len(rows[0])
    flat = [chunk for chunks in rows for chunk in chunks]
    n_cols = sum(c.shape[0] for c in cols)
    height = sum(widths)
    n_in = len(flat)

    def body(*refs):
        row_refs = refs[:n_in]
        col_refs = refs[n_in : n_in + len(cols)]
        o_ref = refs[-1]
        at = 0
        for i, width in enumerate(widths):
            lhs = jnp.concatenate([r[...] for r in row_refs[i * count : (i + 1) * count]], axis=1)
            to = 0
            for c in col_refs:
                n = c.shape[0]
                acc = lax.dot_general(
                    lhs, c[...], (((1,), (1,)), ((), ())), preferred_element_type=jnp.float32
                )
                o_ref[0, at : at + width, to : to + n] = acc * scale
                to += n
            at += width

    in_specs = [
        pl.BlockSpec((width, tokens), lambda m: (m, 0)) for width in widths for _ in range(count)
    ]
    in_specs += [pl.BlockSpec(c.shape, lambda m: (0, 0)) for c in cols]
    operands = flat + list(cols)
    aliases = {}
    if out is not None:
        in_specs.append(ANY)
        operands.append(out)
        aliases = {len(operands) - 1: 0}
    return pl.pallas_call(
        body,
        grid=(panels,),
        out_shape=jax.ShapeDtypeStruct((panels, col_width, col_width), jnp.float32),
        in_specs=in_specs,
        out_specs=pl.BlockSpec((1, height, n_cols), lambda m: (m, row_block, col_start // n_cols)),
        input_output_aliases=aliases,
        cost_estimate=pl.CostEstimate(
            flops=2 * panels * height * n_cols * count * tokens, transcendentals=0, bytes_accessed=0
        ),
        compiler_params=pltpu.CompilerParams(vmem_limit_bytes=48 * 1024 * 1024),
        name=name,
    )(*operands)


def ringed(grad_hidden, gate, col_width):
    tensor_count = lax.axis_size("tensor")
    data_count = lax.axis_size("dp")
    tokens, hidden = grad_hidden.shape
    panels = hidden // col_width
    ratio = data_count // tensor_count
    chips = data_count // 2
    total_tokens = tokens * data_count
    data_index = lax.axis_index("dp")
    owned = data_index // ratio == lax.axis_index("tensor")
    panel = (data_index % ratio).astype(jnp.int32).reshape(1)

    order = list(range(0, chips, 2)) + list(range(1, chips, 2))[::-1]
    around = []
    for i, chip in enumerate(order):
        around.append((2 * chip, 2 * order[(i + 1) % chips]))
        around.append((2 * chip + 1, 2 * order[(i - 1) % chips] + 1))
    partner = [(d, d ^ 1) for d in range(data_count)]
    across = []
    for d in range(data_count):
        own = d // ratio
        across.append((d * tensor_count + own, d * tensor_count + 1 - own))

    def ring(chunk):
        return lax.ppermute(chunk, "dp", around)

    def swap(chunk):
        return lax.ppermute(chunk, "dp", partner)

    widths = []
    left = col_width
    while left > 0:
        widths.append(min(2 * LANES, left))
        left -= widths[-1]
    starts = [sum(widths[:j]) for j in range(len(widths))]

    dep = jnp.zeros((8, LANES), jnp.float32)
    out = None
    rows, cols = [], []
    for j, (start, width) in enumerate(zip(starts, widths)):
        mine = gate_chunk(grad_hidden, gate, dep, col_width, start, width)
        other = swap(mine)
        got = [mine, other]
        a, b = mine, other
        for hop in range(1, chips // 2):
            a = ring(a)
            b = ring(b)
            got += [a, b, swap(a), swap(b)]
            if hop == chips // 2 - 1:
                dep = a
        a = ring(a)
        got += [a, swap(a)]
        piece = pick_panel(got, panel, width)
        sent = lax.ppermute(piece, ("dp", "tensor"), across)
        cols.append(jnp.where(owned, piece, sent))
        rows.append(got)
        row_block = start // width
        make = functools.partial(product, panels=panels, col_width=col_width, scale=1.0 / total_tokens)
        out = make(
            out, [got], cols, widths=[width], col_start=0, row_block=row_block, name=f"rows_{j}"
        )
        if j:
            out = make(
                out, rows[:j], cols[j:], widths=widths[:j], col_start=start, row_block=0, name=f"cols_{j}"
            )
    return out.reshape(hidden, col_width)


def solution(mesh):
    def shards(grad_hidden, gate):
        tokens, hidden = grad_hidden.shape
        data_count, tensor_count = mesh.shape["dp"], mesh.shape["tensor"]
        col_width = hidden * tensor_count // data_count
        total_tokens = tokens * data_count
        fits = (
            tensor_count == 2
            and data_count % 8 == 0
            and data_count % tensor_count == 0
            and col_width % LANES == 0
            and tokens % LANES == 0
            and hidden % col_width == 0
            and total_tokens & (total_tokens - 1) == 0
        )
        return (ringed if fits else gathered)(grad_hidden, gate, col_width)

    return jax.shard_map(
        shards,
        mesh=mesh,
        in_specs=(P("dp", "tensor"), P("dp", "tensor")),
        out_specs=P("tensor", "dp"),
        check_vma=False,
    )
```
